32 devices in a mesh: heads: 2 (over y), ctx: 16 (over z, x, core).
Axes of the slice: x: 2, y: 2, z: 4, core: 2. Of those that a mesh axis runs over, the one named last changes fastest.
Arguments:
- queries: bfloat16 [64, 8192], P('ctx', 'heads'), may hold values from -6 to 6
- keys: bfloat16 [32768, 1024], P('ctx', 'heads'), may hold values from -18 to 18
- values: bfloat16 [32768, 1024], P('ctx', 'heads'), may hold values from -6 to 6
- cache_positions: int32 [32768], P('ctx'), may hold values from 0 to 32767, as said below
- query_positions: int32 [64], P('ctx'), may hold values from 32704 to 32767, as said below
- lengths: int32 [16], P('ctx'), may hold values from 1024 to 2048, as said below
Outputs:
- attended: bfloat16 [64, 8192], P('ctx', 'heads')
The draws below stay inside these ranges and needn't reach their ends.
Inputs may be any that keep to these rules, and one draw needn't show every extreme that they name: `cache_positions`: the values 0 to 32767, each once; slot 0 holds position 0. `query_positions`: the last 64 positions, each once. `lengths`: some block of the cache is full.
All inputs are finite; a program needn't handle non-finite values.
Results may differ from the reference program's by a relative error of at most 0.0055.
Values may be sent and summed in bfloat16 or wider, within the bound.
A program may use at most 64 MiB of HBM per device.

```python
import jax
import jax.numpy as jnp
from jax import lax

HEADS = 64
KVH = 8
HD = 128
GROUP = 8
Q_DEV = 4
CACHE_DEV = 2048
NEW = 64
CACHE = 32768


def slot_places(key):
    shuffled = jax.random.permutation(jax.random.fold_in(key, 11), CACHE).astype(jnp.int32)
    where_zero = jnp.argmin(shuffled).astype(jnp.int32)
    leading = shuffled[0]
    shuffled = shuffled.at[where_zero].set(leading)
    return shuffled.at[0].set(0)


def draw_cache_positions(key, part):
    return slot_places(key)


def draw_query_positions(key, part):
    shuffled = jax.random.permutation(jax.random.fold_in(key, 23), NEW)
    return (CACHE - NEW + shuffled).astype(jnp.int32)


def draw_lengths(key, part):
    shards = CACHE // CACHE_DEV
    counts = jax.random.randint(jax.random.fold_in(key, 31), (shards,), CACHE_DEV // 2, CACHE_DEV + 1)
    filled = jax.random.randint(jax.random.fold_in(key, 37), (), 0, shards)
    return counts.at[filled].set(CACHE_DEV).astype(jnp.int32)


def draw_keys(key, part):
    drawn = jnp.clip(3.0 * jax.random.normal(jax.random.fold_in(key, 53), (CACHE, KVH * HD), jnp.float32), -18.0, 18.0)
    return drawn.astype(jnp.bfloat16)


def draw_queries(key, part):
    drawn = jnp.clip(jax.random.normal(jax.random.fold_in(key, 61), (NEW, HEADS * HD), jnp.float32), -6.0, 6.0)
    return drawn.astype(jnp.bfloat16)


def shard_levels(stream_key, extent, pieces, least, top_value):
    gain, own = 1.0, jax.random.fold_in(stream_key, 6)
    for position, shards_of in pieces:
        steps = jnp.exp(jax.random.uniform(jax.random.fold_in(own, position), (shards_of,), jnp.float32, least / len(pieces), top_value / len(pieces)))
        gain = gain * jnp.repeat(steps, extent[position] // shards_of).reshape([-1 if axis == position else 1 for axis in range(len(extent))])
    return gain


def bell_draw(stream_key, extent, deviation, most, split=(), held_as=jnp.bfloat16):
    array = deviation * jax.random.normal(stream_key, extent, jnp.float32)
    if split:
        array = array * shard_levels(stream_key, extent, split, -0.22, 0.18)
    return jnp.clip(array, -most, most).astype(held_as)


def setup_inputs(seed: int = 0) -> dict:
    key_list = jax.random.split(jax.random.key(seed), 7)
    return {
        "queries": draw_queries(jax.random.fold_in(key_list[6], 71), 0),
        "keys": draw_keys(jax.random.fold_in(key_list[6], 71), 0),
        "values": bell_draw(key_list[2], (CACHE, KVH * HD), 1.0, 6.0, ((0, 16), (1, 2))),
        "cache_positions": draw_cache_positions(jax.random.fold_in(key_list[6], 71), 0),
        "query_positions": draw_query_positions(jax.random.fold_in(key_list[6], 71), 0),
        "lengths": draw_lengths(jax.random.fold_in(key_list[6], 71), 0),
    }


NEG_FILL = -1.0e30


def reference(queries, keys, values, cache_positions, query_positions, lengths):
    slot_ids = jnp.arange(CACHE, dtype=jnp.int32)
    shard_ids = slot_ids // CACHE_DEV
    live_slots = (slot_ids - shard_ids * CACHE_DEV) < lengths[shard_ids]
    blocks = NEW // Q_DEV
    query_split = queries.reshape(blocks, Q_DEV, KVH, GROUP, HD).transpose(2, 0, 1, 3, 4)
    block_places = query_positions.reshape(blocks, Q_DEV)
    key_heads = keys.astype(jnp.float32).reshape(CACHE, KVH, HD).transpose(1, 0, 2)
    value_heads = values.astype(jnp.float32).reshape(CACHE, KVH, HD).transpose(1, 0, 2)
    score_scale = HD ** -0.5

    def per_head(member):
        head_keys, head_values, head_queries = member

        def per_block(block_pair):
            block, places = block_pair
            scores = jnp.einsum("rgd,cd->grc", block.astype(jnp.float32), head_keys) * score_scale
            allowed = live_slots[None, :] & (cache_positions[None, :] <= places[:, None])
            scores = jnp.where(allowed[None], scores, NEG_FILL)
            row_max = jnp.max(scores, axis=2, keepdims=True)
            weights = jnp.where(allowed[None], jnp.exp(scores - row_max), 0.0)
            totals = jnp.sum(weights, axis=2)
            rounded = lax.optimization_barrier(weights.astype(jnp.bfloat16)).astype(jnp.float32)
            weighted = jnp.einsum("grc,cd->rgd", rounded, head_values)
            return weighted / totals.T[:, :, None]

        return lax.map(per_block, (head_queries, block_places))

    result = lax.map(per_head, (key_heads, value_heads, query_split))
    return result.transpose(1, 2, 0, 3, 4).reshape(NEW, HEADS * HD).astype(jnp.bfloat16)
```

```python
import functools
import math

import jax
import jax.numpy as jnp
from jax import lax
from jax.experimental import pallas as pl
from jax.experimental.pallas import tpu as pltpu
from jax.sharding import PartitionSpec as P

HD = 128
GROUP = 8
SUB = 8
NEG_FILL = -1e30
FAR = 2**30
EXP_SCALE = math.log2(math.e) * HD**-0.5


def kernel(
    n,
    lengths_ref, places_ref, queries_ref, slots_ref, keys_ref, values_ref, out_ref,
    heads_f32, q_mine, q_all, p_mine, p_all, k_buf, v_buf, s_buf, bias, o_mine, o_all,
    st_mine, st_all, w_rows, w_cols,
    k_sem, v_sem, pair_send, pair_recv,
    q_send, q_recv, p_send, p_recv, o_send, o_recv, st_send, st_recv,
):
    tok = queries_ref.shape[0]
    rows = tok * GROUP
    slots = keys_ref.shape[0]
    kv_local = keys_ref.shape[1] // HD
    half = kv_local // 2
    width = half * HD
    per = HD // rows
    batches = n // per

    me = lax.axis_index("ctx")
    core = lax.rem(me, 2)
    twin = me + 1 - 2 * core
    my_batch = lax.div(me, per)
    my_place = lax.rem(me, per)

    def to(device):
        return {"ctx": device}

    def remote(src, dst, send, recv, device):
        return pltpu.make_async_remote_copy(
            src_ref=src, dst_ref=dst, send_sem=send, recv_sem=recv,
            device_id=to(device), device_id_type=pl.DeviceIdType.MESH,
        )

    mine_cols = pl.ds(pl.multiple_of(core * width, HD), width)
    twin_cols = pl.ds(pl.multiple_of((1 - core) * width, HD), width)
    own_k = pltpu.make_async_copy(keys_ref.at[:, mine_cols], k_buf.at[0], k_sem)
    own_v = pltpu.make_async_copy(values_ref.at[:, mine_cols], v_buf.at[0], v_sem)

    barrier = pltpu.get_barrier_semaphore()
    for step in range(1, n):
        pl.semaphore_signal(
            barrier, inc=1, device_id=to(lax.rem(me + step, n)),
            device_id_type=pl.DeviceIdType.MESH,
        )
    own_k.start()
    own_v.start()

    wide = queries_ref[...].astype(jnp.float32)
    for kv in range(kv_local):
        for g in range(GROUP):
            col = (kv * GROUP + g) * HD
            heads_f32[kv, g * tok:(g + 1) * tok, :] = wide[:, col:col + HD]
    for c in range(2):
        for h in range(half):
            q_mine[c, h] = heads_f32[c * half + h].astype(jnp.bfloat16)
    sub = lax.rem(lax.broadcasted_iota(jnp.int32, (SUB, HD), 0), tok)
    place = jnp.full((SUB, HD), places_ref[0], jnp.int32)
    for t in range(1, tok):
        place = jnp.where(sub == t, places_ref[t], place)
    p_mine[...] = place
    p_all[me] = place
    q_all[me] = q_mine[core]
    live = lax.broadcasted_iota(jnp.int32, (1, slots), 1) < lengths_ref[0]
    s_buf[0] = jnp.where(live, slots_ref[...], FAR)

    pl.semaphore_wait(barrier, n - 1)

    pair = [
        remote(s_buf.at[0], s_buf.at[1], pair_send.at[0], pair_recv.at[0], twin),
        remote(keys_ref.at[:, twin_cols], k_buf.at[1], pair_send.at[1], pair_recv.at[1], twin),
        remote(values_ref.at[:, twin_cols], v_buf.at[1], pair_send.at[2], pair_recv.at[2], twin),
    ]

    def q_copy(peer, slot):
        return remote(q_mine.at[lax.rem(peer, 2)], q_all.at[slot], q_send.at[peer], q_recv.at[slot], peer)

    def p_copy(peer, slot):
        return remote(p_mine, p_all.at[slot], p_send.at[peer], p_recv.at[slot], peer)

    def peer_at(back, j):
        group = lax.rem(my_batch + batches - back, batches)
        return group * per + lax.rem(my_place + j, per)

    for back in range(batches):
        for j in range(per):
            if back == 0 and j == 0:
                continue
            peer = peer_at(back, j)
            p_copy(peer, me).start()
            q_copy(peer, me).start()
        if back == 0:
            for copy in pair:
                copy.start()

    own_k.wait()
    own_v.wait()
    for copy in pair:
        copy.wait()

    def o_copy(peer, slot):
        return remote(o_mine.at[peer], o_all.at[slot], o_send.at[peer], o_recv.at[slot], peer)

    def st_copy(peer, slot):
        return remote(
            st_mine.at[lax.div(peer, per)], st_all.at[slot], st_send.at[peer], st_recv.at[slot], peer
        )

    def one_batch(ahead, carry):
        group = lax.rem(my_batch + ahead, batches)
        first = group * per
        for j in range(per):
            src = first + j

            @pl.when(src != me)
            def _():
                p_copy(src, src).wait_recv()
                q_copy(src, src).wait_recv()

        for j in range(per):
            at = p_all[first + j]
            for side in range(2):
                far = jnp.concatenate([at] * (slots // HD), axis=1)
                seen = jnp.broadcast_to(s_buf[side], (SUB, slots)) <= far
                bias[j, :, side * slots:(side + 1) * slots] = jnp.where(seen, 0.0, NEG_FILL)

        lane = lax.broadcasted_iota(jnp.int32, (HD, HD), 1)
        stats = jnp.zeros((HD, HD), jnp.float32)
        for h in range(half):
            q = q_all[pl.ds(first, per), h].reshape(HD, HD)
            cols = slice(h * HD, (h + 1) * HD)
            keys = k_buf[:, :, cols].reshape(2 * slots, HD)
            vals = v_buf[:, :, cols].reshape(2 * slots, HD)
            s = lax.dot_general(
                q, keys, (((1,), (1,)), ((), ())), preferred_element_type=jnp.float32
            )
            s = s.reshape(per, rows // SUB, SUB, 2 * slots) + bias[...][:, None]
            s = s.reshape(HD, 2 * slots)
            top = jnp.max(s, axis=1, keepdims=True)
            w = jnp.exp2((s - top) * EXP_SCALE)
            total = jnp.sum(w, axis=1, keepdims=True)
            o = jnp.dot(w.astype(jnp.bfloat16), vals, preferred_element_type=jnp.float32)
            o_mine[pl.ds(first, per), h] = o.astype(jnp.bfloat16).reshape(per, rows, HD)
            stats = jnp.where(lane == h, top, stats)
            stats = jnp.where(lane == half + h, total, stats)
        st_mine[group] = stats.T[:SUB]

        for j in range(per):
            dst = first + lax.rem(my_place + j, per)

            @pl.when(dst != me)
            def _():
                st_copy(dst, me).start()
                o_copy(dst, me).start()

        return carry

    lax.fori_loop(0, batches, one_batch, 0)
    o_all[me] = o_mine[me]
    st_all[me] = st_mine[my_batch]

    for back in range(batches):
        for j in range(per):
            if back == 0 and j == 0:
                continue
            src = peer_at(back, j)
            st_copy(src, src).wait_recv()
            o_copy(src, src).wait_recv()

    for c in range(2):
        members = range(c, n, 2)
        top = functools.reduce(jnp.maximum, [st_all[s, :half] for s in members])
        factors = [jnp.exp2((st_all[s, :half] - top) * EXP_SCALE) for s in members]
        total = functools.reduce(
            jnp.add, [st_all[s, half:2 * half] * f for s, f in zip(members, factors)]
        )
        inverse = 1.0 / total
        for s, f in zip(members, factors):
            w_rows[s * SUB:s * SUB + half, :] = f * inverse
    for at in range(0, n * SUB, HD):
        w_cols[:, at:at + HD] = w_rows[at:at + HD, :].T
    weight = w_cols[pl.ds(pl.multiple_of(my_place * rows, rows), rows), :]
    for c in range(2):
        for h in range(half):
            result = jnp.zeros((rows, HD), jnp.float32)
            for s in range(c, n, 2):
                col = s * SUB + h
                result = result + weight[:, col:col + 1] * o_all[s, h].astype(jnp.float32)
            heads_f32[c * half + h] = result
    for kv in range(kv_local):
        for g in range(GROUP):
            col = (kv * GROUP + g) * HD
            out_ref[:, col:col + HD] = heads_f32[kv, g * tok:(g + 1) * tok, :].astype(jnp.bfloat16)

    for back in range(batches):
        for j in range(per):
            if back == 0 and j == 0:
                continue
            peer = peer_at(back, j)
            p_copy(peer, me).wait_send()
            q_copy(peer, me).wait_send()
            st_copy(peer, me).wait_send()
            o_copy(peer, me).wait_send()


def per_device(n, queries, keys, values, cache_positions, query_positions, lengths):
    tok, wide = queries.shape
    slots = keys.shape[0]
    kv_local = keys.shape[1] // HD
    half = kv_local // 2
    rows = tok * GROUP
    per = HD // rows
    vmem = pl.BlockSpec(memory_space=pltpu.VMEM)
    smem = pl.BlockSpec(memory_space=pltpu.SMEM)
    hbm = pl.BlockSpec(memory_space=pltpu.HBM)
    dma = pltpu.SemaphoreType.DMA
    return pl.pallas_call(
        functools.partial(kernel, n),
        out_shape=jax.ShapeDtypeStruct((tok, wide), jnp.bfloat16),
        in_specs=[smem, smem, vmem, vmem, hbm, hbm],
        out_specs=vmem,
        scratch_shapes=[
            pltpu.VMEM((kv_local, rows, HD), jnp.float32),
            pltpu.VMEM((2, half, rows, HD), jnp.bfloat16),
            pltpu.VMEM((n, half, rows, HD), jnp.bfloat16),
            pltpu.VMEM((SUB, HD), jnp.int32),
            pltpu.VMEM((n, SUB, HD), jnp.int32),
            pltpu.VMEM((2, slots, half * HD), jnp.bfloat16),
            pltpu.VMEM((2, slots, half * HD), jnp.bfloat16),
            pltpu.VMEM((2, 1, slots), jnp.int32),
            pltpu.VMEM((per, SUB, 2 * slots), jnp.float32),
            pltpu.VMEM((n, half, rows, HD), jnp.bfloat16),
            pltpu.VMEM((n, half, rows, HD), jnp.bfloat16),
            pltpu.VMEM((n // per, SUB, HD), jnp.float32),
            pltpu.VMEM((n, SUB, HD), jnp.float32),
            pltpu.VMEM((n * SUB, HD), jnp.float32),
            pltpu.VMEM((HD, n * SUB), jnp.float32),
            dma, dma, dma((3,)), dma((3,)),
            dma((n,)), dma((n,)), dma((n,)), dma((n,)),
            dma((n,)), dma((n,)), dma((n,)), dma((n,)),
        ],
        compiler_params=pltpu.CompilerParams(
            collective_id=0, has_side_effects=True, vmem_limit_bytes=60 * 2**20
        ),
    )(lengths, query_positions, queries, cache_positions.reshape(1, slots), keys, values)


def solution(mesh):
    in_specs = (
        P("ctx", "heads"),
        P("ctx", "heads"),
        P("ctx", "heads"),
        P("ctx"),
        P("ctx"),
        P("ctx"),
    )
    return jax.shard_map(
        functools.partial(per_device, mesh.shape["ctx"]),
        mesh=mesh, in_specs=in_specs, out_specs=P("ctx", "heads"), check_vma=False,
    )
```

```python
import functools
import math

import jax
import jax.numpy as jnp
from jax import lax
from jax.experimental import pallas as pl
from jax.experimental.pallas import tpu as pltpu
from jax.sharding import PartitionSpec as P

HD = 128
GROUP = 8
SUB = 8
NEG_FILL = -1e30
FAR = 2.0**30
EXP_SCALE = math.log2(math.e) * HD**-0.5


def kernel(
    n,
    lengths_ref, places_ref, queries_ref, slots_ref, keys_ref, values_ref, out_ref,
    q_in, heads_f32, q_mine, q_all, p_mine, p_all, k_buf, v_buf, s_buf, bias, o_mine, o_all,
    st_mine, st_all, w_rows,
    q_sem, k_sem, v_sem, pair_send, pair_recv,
    q_send, q_recv, p_send, p_recv, o_send, o_recv, st_send, st_recv,
):
    tok = queries_ref.shape[0]
    rows = tok * GROUP
    slots = keys_ref.shape[0]
    kv_local = keys_ref.shape[1] // HD
    half = kv_local // 2
    width = half * HD
    per = HD // rows
    batches = n // per

    me = lax.axis_index("ctx")
    core = lax.rem(me, 2)
    twin = me + 1 - 2 * core
    my_batch = lax.div(me, per)
    my_place = lax.rem(me, per)

    def to(device):
        return {"ctx": device}

    def remote(src, dst, send, recv, device):
        return pltpu.make_async_remote_copy(
            src_ref=src, dst_ref=dst, send_sem=send, recv_sem=recv,
            device_id=to(device), device_id_type=pl.DeviceIdType.MESH,
        )

    mine_cols = pl.ds(pl.multiple_of(core * width, HD), width)
    twin_cols = pl.ds(pl.multiple_of((1 - core) * width, HD), width)
    own_k = pltpu.make_async_copy(keys_ref.at[:, mine_cols], k_buf.at[0], k_sem)
    own_v = pltpu.make_async_copy(values_ref.at[:, mine_cols], v_buf.at[0], v_sem)

    own_step = batches - 1
    barrier = pltpu.get_barrier_semaphore()
    for step in range(1, n):
        pl.semaphore_signal(
            barrier, inc=1, device_id=to(lax.rem(me + step, n)),
            device_id_type=pl.DeviceIdType.MESH,
        )
    own_q = pltpu.make_async_copy(queries_ref, q_in, q_sem)
    own_q.start()
    own_k.start()
    own_v.start()

    lane_row = lax.broadcasted_iota(jnp.int32, (1, HD), 1)
    place = jnp.zeros((1, HD), jnp.float32)
    for t in range(tok):
        place = jnp.where(lane_row == t, places_ref[t].astype(jnp.float32), place)
    p_mine[...] = place
    p_all[me] = place
    live = lax.broadcasted_iota(jnp.int32, (1, slots), 1) < lengths_ref[0]
    s_buf[0] = jnp.where(live, slots_ref[...].astype(jnp.float32), FAR)

    own_q.wait()
    wide = q_in[...].astype(jnp.float32)
    for kv in range(kv_local):
        for g in range(GROUP):
            col = (kv * GROUP + g) * HD
            heads_f32[kv, g * tok:(g + 1) * tok, :] = wide[:, col:col + HD]
    for c in range(2):
        for h in range(half):
            q_mine[c, h] = heads_f32[c * half + h].astype(jnp.bfloat16)
    q_all[me] = q_mine[core]
    pl.semaphore_wait(barrier, n - 1)

    pair = [
        remote(s_buf.at[0], s_buf.at[1], pair_send.at[0], pair_recv.at[0], twin),
        remote(keys_ref.at[:, twin_cols], k_buf.at[1], pair_send.at[1], pair_recv.at[1], twin),
        remote(values_ref.at[:, twin_cols], v_buf.at[1], pair_send.at[2], pair_recv.at[2], twin),
    ]

    def q_copy(peer, slot):
        return remote(q_mine.at[lax.rem(peer, 2)], q_all.at[slot], q_send.at[peer], q_recv.at[slot], peer)

    def p_copy(peer, slot):
        return remote(p_mine, p_all.at[slot], p_send.at[peer], p_recv.at[slot], peer)

    def group_of(step):
        group, bit = my_batch, 1
        while bit < batches:
            mine = lax.rem(lax.div(my_batch, bit), 2)
            other = lax.rem(lax.div(step + 1, bit), 2)
            group = group + bit * other * (1 - 2 * mine)
            bit *= 2
        return group

    def peer_at(step, j):
        group = group_of(step)
        return group * per + lax.rem(my_place + j, per)

    for back in range(batches):
        for j in range(per):
            if back == own_step and j == 0:
                continue
            peer = peer_at(back, j)
            p_copy(peer, me).start()
            q_copy(peer, me).start()
        if back == 0:
            for copy in pair:
                copy.start()

    own_k.wait()
    own_v.wait()
    for copy in pair:
        copy.wait()

    def o_copy(peer, slot):
        return remote(o_mine.at[peer], o_all.at[slot], o_send.at[peer], o_recv.at[slot], peer)

    def st_copy(peer, slot):
        return remote(
            st_mine.at[peer], st_all.at[slot], st_send.at[peer], st_recv.at[slot], peer
        )

    lane = lax.broadcasted_iota(jnp.int32, (HD, HD), 1)
    token_lane = lax.broadcasted_iota(jnp.int32, (SUB, HD), 1) == lax.rem(
        lax.broadcasted_iota(jnp.int32, (SUB, HD), 0), tok
    )

    def one_batch(ahead, carry):
        group = group_of(ahead)
        first = group * per
        for j in range(per):
            src = first + j

            @pl.when(src != me)
            def _():
                p_copy(src, src).wait_recv()
                q_copy(src, src).wait_recv()

        for j in range(per):
            row = jnp.broadcast_to(p_all[first + j], (SUB, HD))
            at = jnp.max(jnp.where(token_lane, row, -1.0), axis=1, keepdims=True)
            for side in range(2):
                seen = jnp.broadcast_to(s_buf[side], (SUB, slots)) <= at
                bias[j, :, side * slots:(side + 1) * slots] = jnp.where(seen, 0.0, NEG_FILL)

        tops, sums = [], []
        for h in range(half):
            q = q_all[pl.ds(first, per), h].reshape(HD, HD)
            cols = slice(h * HD, (h + 1) * HD)
            keys = k_buf[:, :, cols].reshape(2 * slots, HD)
            vals = v_buf[:, :, cols].reshape(2 * slots, HD)
            s = lax.dot_general(
                q, keys, (((1,), (1,)), ((), ())), preferred_element_type=jnp.float32
            )
            s = s.reshape(per, rows // SUB, SUB, 2 * slots) + bias[...][:, None]
            s = s.reshape(HD, 2 * slots)
            top = jnp.max(s, axis=1, keepdims=True)
            w = jnp.exp2((s - top) * EXP_SCALE)
            total = jnp.sum(w, axis=1, keepdims=True)
            o = jnp.dot(w.astype(jnp.bfloat16), vals, preferred_element_type=jnp.float32)
            o_mine[pl.ds(first, per), h] = o.astype(jnp.bfloat16).reshape(per, rows, HD)
            tops.append(top)
            sums.append(total)
        stats = jnp.zeros((HD, HD), jnp.float32)
        for j in range(per):
            column = jnp.concatenate([v[j * rows:(j + 1) * rows] for v in tops + sums], axis=0)
            stats = jnp.where(lane == j, column, stats)
        stats = stats.T
        for j in range(per):
            st_mine[first + j] = stats[j:j + 1]

        for j in range(per):
            dst = first + lax.rem(my_place + j, per)

            @pl.when(dst != me)
            def _():
                st_copy(dst, me).start()
                o_copy(dst, me).start()

        return carry

    lax.fori_loop(0, batches, one_batch, 0, unroll=min(batches, 4))
    o_all[me] = o_mine[me]
    st_all[me] = st_mine[me]

    for back in range(batches):
        for j in range(per):
            if back == own_step and j == 0:
                continue
            src = peer_at(back, j)
            st_copy(src, src).wait_recv()
            o_copy(src, src).wait_recv()

    sources = n // 2
    w_rows[...] = jnp.zeros_like(w_rows)
    for c in range(2):
        for b in range(sources):
            w_rows[c * sources + b:c * sources + b + 1, :] = st_all[2 * b + c]
    count = half * rows
    spread = w_rows[...].T
    for c in range(2):
        mine = spread[:, c * sources:(c + 1) * sources]
        top = jnp.max(mine[:count], axis=1, keepdims=True)
        factor = jnp.exp2((mine[:count] - top) * EXP_SCALE)
        total = jnp.sum(mine[count:2 * count] * factor, axis=1, keepdims=True)
        factor = factor / total
        for h in range(half):
            span = slice(h * rows, (h + 1) * rows)
            result = jnp.zeros((rows, HD), jnp.float32)
            for b in range(sources):
                result = result + factor[span, b:b + 1] * o_all[2 * b + c, h].astype(jnp.float32)
            heads_f32[c * half + h] = result
    for kv in range(kv_local):
        for g in range(GROUP):
            col = (kv * GROUP + g) * HD
            out_ref[:, col:col + HD] = heads_f32[kv, g * tok:(g + 1) * tok, :].astype(jnp.bfloat16)

    for back in range(batches):
        for j in range(per):
            if back == own_step and j == 0:
                continue
            peer = peer_at(back, j)
            p_copy(peer, me).wait_send()
            q_copy(peer, me).wait_send()
            st_copy(peer, me).wait_send()
            o_copy(peer, me).wait_send()


def per_device(n, queries, keys, values, cache_positions, query_positions, lengths):
    tok, wide = queries.shape
    slots = keys.shape[0]
    kv_local = keys.shape[1] // HD
    half = kv_local // 2
    rows = tok * GROUP
    per = HD // rows
    vmem = pl.BlockSpec(memory_space=pltpu.VMEM)
    smem = pl.BlockSpec(memory_space=pltpu.SMEM)
    hbm = pl.BlockSpec(memory_space=pltpu.HBM)
    dma = pltpu.SemaphoreType.DMA
    return pl.pallas_call(
        functools.partial(kernel, n),
        out_shape=jax.ShapeDtypeStruct((tok, wide), jnp.bfloat16),
        in_specs=[smem, smem, hbm, vmem, hbm, hbm],
        out_specs=vmem,
        scratch_shapes=[
            pltpu.VMEM((tok, wide), jnp.bfloat16),
            pltpu.VMEM((kv_local, rows, HD), jnp.float32),
            pltpu.VMEM((2, half, rows, HD), jnp.bfloat16),
            pltpu.VMEM((n, half, rows, HD), jnp.bfloat16),
            pltpu.VMEM((1, HD), jnp.float32),
            pltpu.VMEM((n, 1, HD), jnp.float32),
            pltpu.VMEM((2, slots, half * HD), jnp.bfloat16),
            pltpu.VMEM((2, slots, half * HD), jnp.bfloat16),
            pltpu.VMEM((2, 1, slots), jnp.float32),
            pltpu.VMEM((per, SUB, 2 * slots), jnp.float32),
            pltpu.VMEM((n, half, rows, HD), jnp.bfloat16),
            pltpu.VMEM((n, half, rows, HD), jnp.bfloat16),
            pltpu.VMEM((n, 1, HD), jnp.float32),
            pltpu.VMEM((n, 1, HD), jnp.float32),
            pltpu.VMEM((pl.cdiv(n, HD) * HD, HD), jnp.float32),
            dma, dma, dma, dma((3,)), dma((3,)),
            dma((n,)), dma((n,)), dma((n,)), dma((n,)),
            dma((n,)), dma((n,)), dma((n,)), dma((n,)),
        ],
        compiler_params=pltpu.CompilerParams(
            collective_id=0, has_side_effects=True, vmem_limit_bytes=60 * 2**20
        ),
    )(lengths, query_positions, queries, cache_positions.reshape(1, slots), keys, values)


def solution(mesh):
    in_specs = (
        P("ctx", "heads"),
        P("ctx", "heads"),
        P("ctx", "heads"),
        P("ctx"),
        P("ctx"),
        P("ctx"),
    )
    return jax.shard_map(
        functools.partial(per_device, mesh.shape["ctx"]),
        mesh=mesh, in_specs=in_specs, out_specs=P("ctx", "heads"), check_vma=False,
    )
```
